16 devices in a mesh: dp: 1, ep: 16 (over x, y, z, core).
Axes of the slice: x: 2, y: 2, z: 2, core: 2. Of those that a mesh axis runs over, the one named last changes fastest.
Arguments:
- x: bfloat16 [1, 16, 256, 3584], P('dp', 'ep')
- expert: int32 [1, 16, 256, 8], P('dp', 'ep')
- slot: int32 [1, 16, 256, 8], P('dp', 'ep')
- gate: float32 [1, 16, 256, 8], P('dp', 'ep')
- w_gate: bfloat16 [32, 3584, 2560], P('ep')
- w_up: bfloat16 [32, 3584, 2560], P('ep')
- w_down: bfloat16 [32, 2560, 3584], P('ep')
- s_gate: bfloat16 [3584, 20480], replicated
- s_up: bfloat16 [3584, 20480], replicated
- s_down: bfloat16 [20480, 3584], replicated
Outputs:
- y: bfloat16 [1, 16, 256, 3584], P('dp', 'ep')
All inputs are finite; a program needn't handle non-finite values.
Results may differ from the reference program's by a relative error of at most 0.009.
Values are sent between devices in bfloat16 or wider.
A program may use at most 2 GiB of HBM per device.

```python
import jax
import jax.numpy as jnp

MEMBERS = 16
TOKENS = 256
D = 3584
FF = 2560
TOP = 8
EXPERTS = 32
SHARED_FF = 20480
SLOTS = 5 * TOKENS * TOP // (4 * EXPERTS)


def setup_inputs(seed: int = 0, part: int = 0) -> dict:
    own, k1, k2, k3, k4, k5, k6 = jax.random.split(jax.random.key(seed), 7)
    kx, ke, kl, kg = jax.random.split(jax.random.fold_in(own, part), 4)
    devices = (1, MEMBERS)
    place = jax.random.permutation(kl, jnp.arange(EXPERTS, dtype=jnp.uint32))
    slow = ((EXPERTS + (9 * place) % EXPERTS) << ((9 * place) // EXPERTS)) // EXPERTS
    wait = (jax.random.bits(ke, (*devices, TOKENS, EXPERTS), jnp.uint32) >> 10) * slow
    expert = jnp.argsort(wait, axis=-1)[..., :TOP].astype(jnp.int32)
    chosen = jax.nn.one_hot(expert, EXPERTS, dtype=jnp.int32)
    in_line = jnp.cumsum(chosen.reshape(*devices, TOKENS * TOP, EXPERTS), axis=2) - 1
    slot = jnp.sum(in_line.reshape(chosen.shape) * chosen, axis=-1)

    def one(key, rows, columns):
        return (jax.random.normal(key, (rows, columns), jnp.float32) * rows**-0.5).astype(jnp.bfloat16)

    def weights(key, rows, columns):
        return jax.lax.map(lambda k: one(k, rows, columns), jax.random.split(key, EXPERTS))

    return {
        "x": jax.random.normal(kx, (*devices, TOKENS, D), jnp.float32).astype(jnp.bfloat16),
        "expert": expert,
        "slot": slot,
        "gate": jax.nn.softmax(jax.random.normal(kg, expert.shape, jnp.float32)),
        "w_gate": weights(k1, D, FF),
        "w_up": weights(k2, D, FF),
        "w_down": weights(k3, FF, D),
        "s_gate": one(k4, D, SHARED_FF),
        "s_up": one(k5, D, SHARED_FF),
        "s_down": one(k6, SHARED_FF, D),
    }


def einsum(form, a, b):
    return jnp.einsum(form, a.astype(jnp.float32), b.astype(jnp.float32))


def for_all(x, s_gate, s_up, s_down):
    h = jax.nn.silu(einsum("...d,df->...f", x, s_gate)) * einsum("...d,df->...f", x, s_up)
    return einsum("...f,fd->...d", h.astype(jnp.bfloat16), s_down)


def reference(x, expert, slot, gate, w_gate, w_up, w_down, s_gate, s_up, s_down):
    to_expert = jax.nn.one_hot(expert, EXPERTS, dtype=jnp.bfloat16)
    to_slot = jax.nn.one_hot(slot, SLOTS, dtype=jnp.bfloat16)
    weighted = to_expert * gate[..., None].astype(jnp.bfloat16)
    dispatch = einsum("abtke,abtkc->abtec", to_expert, to_slot).astype(jnp.bfloat16)
    combine = einsum("abtke,abtkc->abtec", weighted, to_slot).astype(jnp.bfloat16)
    z = einsum("abtec,abtd->aebcd", dispatch, x).astype(jnp.bfloat16)
    h = jax.nn.silu(einsum("aebcd,edf->aebcf", z, w_gate))
    h = (h * einsum("aebcd,edf->aebcf", z, w_up)).astype(jnp.bfloat16)
    out = einsum("aebcf,efd->aebcd", h, w_down).astype(jnp.bfloat16)
    y = einsum("abtec,aebcd->abtd", combine, out)
    return (y + for_all(x, s_gate, s_up, s_down)).astype(jnp.bfloat16)
```

```python
import functools

import jax
import jax.numpy as jnp
from jax import lax
from jax.experimental import pallas as pl
from jax.experimental.pallas import tpu as pltpu
from jax.sharding import PartitionSpec as P


D = 3584
FF = 2560
SFF = 20480
TOP = 8
SLOTS = 80
NDEV = 16
CHIPS = 8
TOK = 256
CHUNKS = 2
CT = TOK // CHUNKS
GROUP = 8
WIN = SLOTS + 16
CAP = NDEV * SLOTS
ZROWS = CAP + 96
PASS = 6
FB = 512
NB = FF // FB
SB = 512
SA_BLOCKS = 19
VMEM = 64 * 1024 * 1024 - 65536


def shared_kernel(x_ref, wg_ref, wu_ref, wd_ref, acc_in, acc_ref, *, first):
    j = pl.program_id(0)

    @pl.when(j == 0)
    def _():
        if first:
            acc_ref[...] = jnp.zeros_like(acc_ref)
        else:
            acc_ref[...] = acc_in[...]

    x = x_ref[...]
    g = jnp.dot(x, wg_ref[...], preferred_element_type=jnp.float32)
    u = jnp.dot(x, wu_ref[...], preferred_element_type=jnp.float32)
    h = (jax.nn.silu(g) * u).astype(jnp.bfloat16)
    acc_ref[...] += jnp.dot(h, wd_ref[...], preferred_element_type=jnp.float32)


def shared(x, wg, wu, wd, start, count, acc=None):
    first = acc is None
    rows = x.shape[0]
    if first:
        acc = jnp.zeros((8, 128), jnp.float32)
        acc_spec = pl.BlockSpec((8, 128), lambda j: (0, 0))
    else:
        acc_spec = pl.BlockSpec((rows, D), lambda j: (0, 0))
    return pl.pallas_call(
        functools.partial(shared_kernel, first=first),
        grid=(count,),
        in_specs=[
            pl.BlockSpec((rows, D), lambda j: (0, 0)),
            pl.BlockSpec((D, SB), lambda j: (0, start + j)),
            pl.BlockSpec((D, SB), lambda j: (0, start + j)),
            pl.BlockSpec((SB, D), lambda j: (start + j, 0)),
            acc_spec,
        ],
        out_specs=pl.BlockSpec((rows, D), lambda j: (0, 0)),
        out_shape=jax.ShapeDtypeStruct((rows, D), jnp.float32),
        compiler_params=pltpu.CompilerParams(vmem_limit_bytes=VMEM),
        cost_estimate=pl.CostEstimate(
            flops=6 * rows * D * SB * count, bytes_accessed=6 * D * SB * count, transcendentals=rows * SB * count
        ),
        name="shared",
    )(x, wg, wu, wd, acc)


def routed_kernel(
    base_ref, off_ref, tiles_ref, core_ref, x_hbm, meta_ref, wg_ref, wu_ref, wd_ref, keep_hbm, away_hbm,
    zbuf, acc, xbuf, abuf, xsem, ksem, asem
):
    e, p, j = pl.program_id(0), pl.program_id(1), pl.program_id(2)
    mc = core_ref[0]

    def source(k, away):
        return 2 * k + (1 - mc if away else mc)

    def fetch(a, slot):
        return pltpu.make_async_copy(x_hbm.at[a], xbuf.at[slot], xsem.at[slot])

    @pl.when((e == 0) & (p == 0) & (j == 0))
    def _():
        fetch(0, 0).start()
        zbuf[...] = jnp.zeros_like(zbuf)

        def step(a, c):
            slot = lax.rem(a, 2)

            @pl.when(a < NDEV - 1)
            def _():
                fetch(a + 1, 1 - slot).start()

            fetch(a, slot).wait()
            m = meta_ref[a]
            rows = lax.broadcasted_iota(jnp.int32, (WIN, CT), 0).astype(jnp.float32)
            for q in range(2):
                pick = jnp.where(m[q : q + 1, :] == rows, 1.0, 0.0).astype(jnp.bfloat16)
                new = jnp.dot(pick, xbuf[slot], preferred_element_type=jnp.float32)
                base = pl.multiple_of(base_ref[q, a], 16)
                row = lax.broadcasted_iota(jnp.int32, (16, 1), 0)
                old = zbuf[q, pl.ds(base, 16), :].astype(jnp.float32)
                zbuf[q, pl.ds(base, 16), :] = jnp.where(row < off_ref[q, a], old, new[:16]).astype(jnp.bfloat16)
                zbuf[q, pl.ds(base + 16, WIN - 16), :] = new[16:].astype(jnp.bfloat16)
            return c

        lax.fori_loop(0, NDEV, step, 0)

    first = p * PASS * 128

    def ffn(start, size):
        z = zbuf[e, pl.ds(pl.multiple_of(first + start, 128), size), :]
        g = jnp.dot(z, wg_ref[0], preferred_element_type=jnp.float32)
        u = jnp.dot(z, wu_ref[0], preferred_element_type=jnp.float32)
        h = (jax.nn.silu(g) * u).astype(jnp.bfloat16)
        acc[pl.ds(start, size), :] += jnp.dot(h, wd_ref[0], preferred_element_type=jnp.float32)

    n = jnp.clip(tiles_ref[e] - p * PASS, 0, PASS)

    @pl.when(j == 0)
    def _():
        def clear(r, c):
            acc[pl.ds(pl.multiple_of(r * 128, 128), 128), :] = jnp.zeros((128, D), jnp.float32)
            return c

        lax.fori_loop(0, n, clear, 0)

    def big(r, c):
        ffn(pl.multiple_of(r * 512, 512), 512)
        return c

    lax.fori_loop(0, n // 4, big, 0)

    @pl.when(lax.rem(n // 2, 2) == 1)
    def _():
        ffn(pl.multiple_of(n // 4 * 512, 128), 256)

    @pl.when(lax.rem(n, 2) == 1)
    def _():
        ffn(pl.multiple_of((n - 1) * 128, 128), 128)

    @pl.when(j == NB - 1)
    def _():
        def keep(r, c):
            rows = acc[pl.ds(pl.multiple_of(r * 128, 128), 128), :]
            zbuf[e, pl.ds(pl.multiple_of(first + r * 128, 128), 128), :] = rows.astype(jnp.bfloat16)
            return c

        lax.fori_loop(0, n, keep, 0)

    @pl.when((e == 1) & (p == 1) & (j == NB - 1))
    def _():
        rows = lax.broadcasted_iota(jnp.int32, (WIN, CT), 0).astype(jnp.float32)

        def put_keep(k, slot):
            return pltpu.make_async_copy(acc.at[pl.ds(slot * CT, CT)], keep_hbm.at[k], ksem.at[slot])

        def put_away(k, slot):
            return pltpu.make_async_copy(abuf.at[slot], away_hbm.at[k], asem.at[slot])

        def result(a):
            m = meta_ref[a]
            total = None
            for q in range(2):
                w = jnp.where(m[q : q + 1, :] == rows, m[2 + q : 3 + q, :], 0.0).astype(jnp.bfloat16)
                base = pl.multiple_of(base_ref[q, a], 16)
                t = lax.dot_general(
                    w, zbuf[q, pl.ds(base, WIN), :], (((0,), (0,)), ((), ())), preferred_element_type=jnp.float32
                )
                total = t if total is None else total + t
            return total

        def step(k, c):
            slot = lax.rem(k, 2)

            @pl.when(k >= 2)
            def _():
                put_away(k - 2, slot).wait()
                put_keep(k - 2, slot).wait()

            abuf[slot] = result(source(k, True)).astype(jnp.bfloat16)
            put_away(k, slot).start()
            acc[pl.ds(pl.multiple_of(slot * CT, CT), CT), :] = result(source(k, False))
            put_keep(k, slot).start()
            return c

        lax.fori_loop(0, CHIPS, step, 0)
        for k in (CHIPS - 2, CHIPS - 1):
            put_away(k, k % 2).wait()
            put_keep(k, k % 2).wait()


def block(e, p, j, tiles):
    return jnp.where(tiles[e] > p * PASS, j, NB - 1)


def routed(base, off, tiles, core, x_all, meta, wg, wu, wd):
    grid_spec = pltpu.PrefetchScalarGridSpec(
        num_scalar_prefetch=4,
        grid=(2, 2, NB),
        in_specs=[
            pl.BlockSpec(memory_space=pl.ANY),
            pl.BlockSpec((NDEV, 8, CT), lambda e, p, j, *_: (0, 0, 0)),
            pl.BlockSpec((1, D, FB), lambda e, p, j, b, o, t, c: (e, 0, block(e, p, j, t))),
            pl.BlockSpec((1, D, FB), lambda e, p, j, b, o, t, c: (e, 0, block(e, p, j, t))),
            pl.BlockSpec((1, FB, D), lambda e, p, j, b, o, t, c: (e, block(e, p, j, t), 0)),
        ],
        out_specs=[pl.BlockSpec(memory_space=pl.ANY), pl.BlockSpec(memory_space=pl.ANY)],
        scratch_shapes=[
            pltpu.VMEM((2, ZROWS, D), jnp.bfloat16),
            pltpu.VMEM((PASS * 128, D), jnp.float32),
            pltpu.VMEM((2, CT, D), jnp.bfloat16),
            pltpu.VMEM((2, CT, D), jnp.bfloat16),
            pltpu.SemaphoreType.DMA((2,)),
            pltpu.SemaphoreType.DMA((2,)),
            pltpu.SemaphoreType.DMA((2,)),
        ],
    )
    return pl.pallas_call(
        routed_kernel,
        grid_spec=grid_spec,
        out_shape=[
            jax.ShapeDtypeStruct((CHIPS, CT, D), jnp.float32),
            jax.ShapeDtypeStruct((CHIPS, CT, D), jnp.bfloat16),
        ],
        compiler_params=pltpu.CompilerParams(vmem_limit_bytes=VMEM),
        cost_estimate=pl.CostEstimate(
            flops=6 * 1280 * D * FF, bytes_accessed=12 * D * FF, transcendentals=1280 * FF
        ),
        name="routed",
    )(base, off, tiles, core, x_all, meta, wg, wu, wd)


def positions(codes, gates, me):
    out = []
    mine = (2 * me + jnp.arange(2)).astype(jnp.float32)
    hit = codes[:, None].astype(jnp.float32) == mine[None, :, None, None, None]
    chosen = jnp.sum(hit.astype(jnp.float32), axis=2)
    weight = jnp.sum(jnp.where(hit, gates[:, None].astype(jnp.float32), 0.0), axis=2)
    before = jnp.triu(jnp.ones((CT, CT), jnp.bfloat16), 1)
    rank = jnp.einsum(
        "aect,tu->aecu", chosen.astype(jnp.bfloat16), before, preferred_element_type=jnp.float32
    )
    count = jnp.sum(chosen, axis=3).astype(jnp.int32)
    end = jnp.cumsum(count, axis=0)
    begin = end - count
    off = lax.rem(begin, 16)
    base = begin - off
    pos = jnp.where(chosen > 0, rank + off[..., None].astype(jnp.float32), -1.0)
    tiles = (end[-1] + 127) // 128
    for c in range(CHUNKS):
        meta = jnp.concatenate(
            [pos[:, :, c], weight[:, :, c], jnp.zeros((NDEV, 4, CT), jnp.float32)], axis=1
        )
        out.append((base[:, :, c].T, off[:, :, c].T, tiles[:, c], meta))
    return out


def solution(mesh):
    def layer(x, expert, slot, gate, w_gate, w_up, w_down, s_gate, s_up, s_down):
        x, expert, slot, gate = x[0, 0], expert[0, 0], slot[0, 0], gate[0, 0]
        me = lax.axis_index("ep")
        core = lax.rem(me, 2)
        chip = me // 2

        code = jnp.where(slot < SLOTS, expert, 32).astype(jnp.bfloat16)
        packed = jnp.concatenate([code, gate.astype(jnp.bfloat16)], axis=1)
        packed = packed.reshape(TOK // (GROUP * CHUNKS), CHUNKS, GROUP, 2 * TOP)
        packed = packed.transpose(3, 1, 0, 2).reshape(2 * TOP, TOK)
        allm = lax.all_gather(packed, "ep", axis=0).reshape(NDEV, 2 * TOP, CHUNKS, CT)
        plan = positions(allm[:, :TOP], allm[:, TOP:], me)

        xs = x.reshape(TOK // (GROUP * CHUNKS), CHUNKS, GROUP, D)
        gathered = [
            lax.all_gather(xs[:, c].reshape(CT, D), "ep", axis=0) for c in range(CHUNKS)
        ]
        acc = shared(x, s_gate, s_up, s_down, 0, SA_BLOCKS)
        parts = []
        pair = [(i, i ^ 1) for i in range(NDEV)]
        groups = [[2 * k + c for k in range(CHIPS)] for c in range(2)]
        after = acc
        for c in range(CHUNKS):
            base, off, tiles, meta = plan[c]
            tokens, after = lax.optimization_barrier((gathered[c], after))
            if c == 0:
                acc = after
            else:
                parts[-1] = (parts[-1][0], after)
            keep, away = routed(base, off, tiles, core[None], tokens, meta, w_gate, w_up, w_down)
            got = lax.ppermute(away, "ep", pair)
            total = (keep + got.astype(jnp.float32)).astype(jnp.bfloat16)
            own = lax.dynamic_index_in_dim(keep, chip, 0, keepdims=False)
            own = own + lax.dynamic_index_in_dim(got, chip, 0, keepdims=False).astype(jnp.float32)
            parts.append((own, total))
            after = total
        x, acc, last = lax.optimization_barrier((x, acc, after))
        parts[-1] = (parts[-1][0], last)
        for c in range(CHUNKS):
            back = lax.all_to_all(parts[c][1], "ep", 0, 0, axis_index_groups=groups, tiled=True)
            parts[c] = (parts[c][0], back)
        rest = shared(x, s_gate, s_up, s_down, SA_BLOCKS, SFF // SB - SA_BLOCKS, acc)
        rest = rest.reshape(TOK // (GROUP * CHUNKS), CHUNKS, GROUP, D)
        outs = []
        others = (jnp.arange(CHIPS) != chip)[:, None, None]
        for c in range(CHUNKS):
            own, back = parts[c]
            t = own + jnp.sum(jnp.where(others, back.astype(jnp.float32), 0.0), axis=0)
            outs.append(t.reshape(TOK // (GROUP * CHUNKS), GROUP, D) + rest[:, c])
        y = jnp.stack(outs, axis=1).reshape(TOK, D).astype(jnp.bfloat16)
        return y[None, None]

    row = P("dp", "ep", None, None)
    return jax.shard_map(
        layer,
        mesh=mesh,
        in_specs=(row, row, row, row) + (P("ep", None, None),) * 3 + (P(None, None),) * 3,
        out_specs=row,
        check_vma=False,
    )
```

```python
import functools

import jax
import jax.numpy as jnp
from jax import lax
from jax.experimental import pallas as pl
from jax.experimental.pallas import tpu as pltpu
from jax.sharding import PartitionSpec as P


D = 3584
FF = 2560
SFF = 20480
TOP = 8
SLOTS = 80
NDEV = 16
CHIPS = 8
TOK = 256
CHUNKS = 2
CT = TOK // CHUNKS
GROUP = 8
WIN = SLOTS + 16
CAP = NDEV * SLOTS
ZROWS = CAP + 96
PASS = 6
FB = 512
NB = FF // FB
SB = 512
SA_BLOCKS = 8
VMEM = 64 * 1024 * 1024 - 65536


def shared_kernel(start_ref, x_ref, wg_ref, wu_ref, wd_ref, acc_in, *rest, last):
    j = pl.program_id(0)
    acc_ref = rest[-1]

    @pl.when(j == 0)
    def _():
        if last:
            acc_ref[...] = acc_in[...]
        else:
            acc_ref[...] = jnp.zeros_like(acc_ref)

    x = x_ref[...]
    g = jnp.dot(x, wg_ref[...], preferred_element_type=jnp.float32)
    u = jnp.dot(x, wu_ref[...], preferred_element_type=jnp.float32)
    h = (jax.nn.silu(g) * u).astype(jnp.bfloat16)
    acc_ref[...] += jnp.dot(h, wd_ref[...], preferred_element_type=jnp.float32)
    if last:
        own_ref, other_ref = rest[:2]

        @pl.when(j == pl.num_programs(0) - 1)
        def _():
            own_ref[...] = acc_ref[:TOK, :]
            other_ref[...] = acc_ref[TOK:, :].astype(jnp.bfloat16)


def shared(x, wg, wu, wd, start, count, acc=None):
    rows = 2 * TOK
    last = acc is not None
    whole = pl.BlockSpec((rows, D), lambda j, s: (0, 0))
    if last:
        acc_spec = whole
        out_specs = [pl.BlockSpec((TOK, D), lambda j, s: (0, 0))] * 2
        out_shape = [jax.ShapeDtypeStruct((TOK, D), jnp.float32), jax.ShapeDtypeStruct((TOK, D), jnp.bfloat16)]
        scratch = [pltpu.VMEM((rows, D), jnp.float32)]
    else:
        acc = jnp.zeros((8, 128), jnp.float32)
        acc_spec = pl.BlockSpec((8, 128), lambda j, s: (0, 0))
        out_specs, out_shape, scratch = whole, jax.ShapeDtypeStruct((rows, D), jnp.float32), []
    return pl.pallas_call(
        functools.partial(shared_kernel, last=last),
        grid_spec=pltpu.PrefetchScalarGridSpec(
            num_scalar_prefetch=1,
            grid=(count,),
            in_specs=[
                whole,
                pl.BlockSpec((D, SB), lambda j, s: (0, s[0] + j)),
                pl.BlockSpec((D, SB), lambda j, s: (0, s[0] + j)),
                pl.BlockSpec((SB, D), lambda j, s: (s[0] + j, 0)),
                acc_spec,
            ],
            out_specs=out_specs,
            scratch_shapes=scratch,
        ),
        out_shape=out_shape,
        compiler_params=pltpu.CompilerParams(vmem_limit_bytes=VMEM),
        cost_estimate=pl.CostEstimate(
            flops=6 * rows * D * SB * count, bytes_accessed=6 * D * SB * count, transcendentals=rows * SB * count
        ),
        name="shared",
    )(start, x, wg, wu, wd, acc)


def final_kernel(chip_ref, own_ref, other_ref, *rest):
    y_ref = rest[-1]
    chip = chip_ref[0]
    sums = []
    for c in range(CHUNKS):
        back_ref, keep_ref, got_ref = rest[3 * c : 3 * c + 3]
        t = keep_ref[0] + got_ref[0].astype(jnp.float32)
        for k in range(CHIPS):
            t += jnp.where(chip == k, 0.0, back_ref[k].astype(jnp.float32))
        sums.append(t)
    pieces = []
    for g in range(16 // GROUP):
        for c in range(CHUNKS):
            pieces.append(sums[c][g * GROUP : (g + 1) * GROUP])
    t = jnp.concatenate(pieces, axis=0)
    y_ref[...] = (t + (own_ref[...] + other_ref[...].astype(jnp.float32))).astype(jnp.bfloat16)


def final(chip, own, other, parts):
    rows = 16 * CHUNKS
    specs = [pl.BlockSpec((rows, D), lambda i, c: (i, 0))] * 2
    args = [own, other]
    for back, keep, got in parts:
        specs.append(pl.BlockSpec((CHIPS, 16, D), lambda i, c: (0, i, 0)))
        specs += [pl.BlockSpec((1, 16, D), lambda i, c: (c[0], i, 0))] * 2
        args += [back, keep, got]
    return pl.pallas_call(
        final_kernel,
        grid_spec=pltpu.PrefetchScalarGridSpec(
            num_scalar_prefetch=1,
            grid=(TOK // rows,),
            in_specs=specs,
            out_specs=pl.BlockSpec((rows, D), lambda i, c: (i, 0)),
        ),
        out_shape=jax.ShapeDtypeStruct((TOK, D), jnp.bfloat16),
        compiler_params=pltpu.CompilerParams(vmem_limit_bytes=40 * 1024 * 1024),
        cost_estimate=pl.CostEstimate(flops=20 * TOK * D, bytes_accessed=24 * CHIPS * TOK * D, transcendentals=0),
        name="final",
    )(chip, *args)


def routed_kernel(
    base_ref, off_ref, tiles_ref, core_ref, x_hbm, meta_ref, wg_ref, wu_ref, wd_ref, keep_hbm, away_hbm,
    zbuf, acc, xbuf, abuf, xsem, ksem, asem
):
    e, p, j = pl.program_id(0), pl.program_id(1), pl.program_id(2)
    mc = core_ref[0]

    def source(k, away):
        return 2 * k + (1 - mc if away else mc)

    def fetch(a, slot):
        return pltpu.make_async_copy(x_hbm.at[a], xbuf.at[slot], xsem.at[slot])

    @pl.when((e == 0) & (p == 0) & (j == 0))
    def _():
        fetch(0, 0).start()
        zbuf[...] = jnp.zeros_like(zbuf)

        def step(a, c):
            slot = lax.rem(a, 2)

            @pl.when(a < NDEV - 1)
            def _():
                fetch(a + 1, 1 - slot).start()

            fetch(a, slot).wait()
            m = meta_ref[a]
            rows = lax.broadcasted_iota(jnp.int32, (WIN, CT), 0).astype(jnp.float32)
            pick = [jnp.where(m[q : q + 1, :] == rows, 1.0, 0.0) for q in range(2)]
            pick = jnp.concatenate(pick, axis=0).astype(jnp.bfloat16)
            both = jnp.dot(pick, xbuf[slot], preferred_element_type=jnp.float32)
            row = lax.broadcasted_iota(jnp.int32, (16, 1), 0)
            for q in range(2):
                new = both[q * WIN : (q + 1) * WIN]
                base = pl.multiple_of(base_ref[q, a], 16)
                old = zbuf[q, pl.ds(base, 16), :].astype(jnp.float32)
                zbuf[q, pl.ds(base, 16), :] = jnp.where(row < off_ref[q, a], old, new[:16]).astype(jnp.bfloat16)
                zbuf[q, pl.ds(base + 16, WIN - 16), :] = new[16:].astype(jnp.bfloat16)
            return c

        lax.fori_loop(0, NDEV, step, 0)

    first = p * PASS * 128

    def ffn(start, size):
        z = zbuf[e, pl.ds(pl.multiple_of(first + start, 128), size), :]
        g = jnp.dot(z, wg_ref[0], preferred_element_type=jnp.float32)
        u = jnp.dot(z, wu_ref[0], preferred_element_type=jnp.float32)
        h = (jax.nn.silu(g) * u).astype(jnp.bfloat16)
        acc[pl.ds(start, size), :] += jnp.dot(h, wd_ref[0], preferred_element_type=jnp.float32)

    n = jnp.clip(tiles_ref[e] - p * PASS, 0, PASS)

    @pl.when(j == 0)
    def _():
        def clear(r, c):
            acc[pl.ds(pl.multiple_of(r * 128, 128), 128), :] = jnp.zeros((128, D), jnp.float32)
            return c

        lax.fori_loop(0, n, clear, 0)

    def big(r, c):
        ffn(pl.multiple_of(r * 512, 512), 512)
        return c

    lax.fori_loop(0, n // 4, big, 0)

    @pl.when(lax.rem(n // 2, 2) == 1)
    def _():
        ffn(pl.multiple_of(n // 4 * 512, 128), 256)

    @pl.when(lax.rem(n, 2) == 1)
    def _():
        ffn(pl.multiple_of((n - 1) * 128, 128), 128)

    @pl.when(j == NB - 1)
    def _():
        def keep(r, c):
            rows = acc[pl.ds(pl.multiple_of(r * 128, 128), 128), :]
            zbuf[e, pl.ds(pl.multiple_of(first + r * 128, 128), 128), :] = rows.astype(jnp.bfloat16)
            return c

        lax.fori_loop(0, n, keep, 0)

    @pl.when((e == 1) & (p == 1) & (j == NB - 1))
    def _():
        rows = lax.broadcasted_iota(jnp.int32, (WIN, CT), 0).astype(jnp.float32)

        def put_keep(k, slot):
            return pltpu.make_async_copy(acc.at[pl.ds(slot * CT, CT)], keep_hbm.at[k], ksem.at[slot])

        def put_away(k, slot):
            return pltpu.make_async_copy(abuf.at[slot], away_hbm.at[k], asem.at[slot])

        def result(a):
            m = meta_ref[a]
            total = None
            for q in range(2):
                w = jnp.where(m[q : q + 1, :] == rows, m[2 + q : 3 + q, :], 0.0).astype(jnp.bfloat16)
                base = pl.multiple_of(base_ref[q, a], 16)
                t = lax.dot_general(
                    w, zbuf[q, pl.ds(base, WIN), :], (((0,), (0,)), ((), ())), preferred_element_type=jnp.float32
                )
                total = t if total is None else total + t
            return total

        def step(k, c):
            slot = lax.rem(k, 2)

            @pl.when(k >= 2)
            def _():
                put_away(k - 2, slot).wait()
                put_keep(k - 2, slot).wait()

            abuf[slot] = result(source(k, True)).astype(jnp.bfloat16)
            put_away(k, slot).start()
            acc[pl.ds(pl.multiple_of(slot * CT, CT), CT), :] = result(source(k, False))
            put_keep(k, slot).start()
            return c

        lax.fori_loop(0, CHIPS, step, 0)
        for k in (CHIPS - 2, CHIPS - 1):
            put_away(k, k % 2).wait()
            put_keep(k, k % 2).wait()


def block(e, p, j, tiles):
    return jnp.where(tiles[e] > p * PASS, j, NB - 1)


def routed(base, off, tiles, core, x_all, meta, wg, wu, wd):
    grid_spec = pltpu.PrefetchScalarGridSpec(
        num_scalar_prefetch=4,
        grid=(2, 2, NB),
        in_specs=[
            pl.BlockSpec(memory_space=pl.ANY),
            pl.BlockSpec((NDEV, 8, CT), lambda e, p, j, *_: (0, 0, 0)),
            pl.BlockSpec((1, D, FB), lambda e, p, j, b, o, t, c: (e, 0, block(e, p, j, t))),
            pl.BlockSpec((1, D, FB), lambda e, p, j, b, o, t, c: (e, 0, block(e, p, j, t))),
            pl.BlockSpec((1, FB, D), lambda e, p, j, b, o, t, c: (e, block(e, p, j, t), 0)),
        ],
        out_specs=[pl.BlockSpec(memory_space=pl.ANY), pl.BlockSpec(memory_space=pl.ANY)],
        scratch_shapes=[
            pltpu.VMEM((2, ZROWS, D), jnp.bfloat16),
            pltpu.VMEM((PASS * 128, D), jnp.float32),
            pltpu.VMEM((2, CT, D), jnp.bfloat16),
            pltpu.VMEM((2, CT, D), jnp.bfloat16),
            pltpu.SemaphoreType.DMA((2,)),
            pltpu.SemaphoreType.DMA((2,)),
            pltpu.SemaphoreType.DMA((2,)),
        ],
    )
    return pl.pallas_call(
        routed_kernel,
        grid_spec=grid_spec,
        out_shape=[
            jax.ShapeDtypeStruct((CHIPS, CT, D), jnp.float32),
            jax.ShapeDtypeStruct((CHIPS, CT, D), jnp.bfloat16),
        ],
        compiler_params=pltpu.CompilerParams(vmem_limit_bytes=VMEM),
        cost_estimate=pl.CostEstimate(
            flops=6 * 1280 * D * FF, bytes_accessed=12 * D * FF, transcendentals=1280 * FF
        ),
        name="routed",
    )(base, off, tiles, core, x_all, meta, wg, wu, wd)


def positions(codes, gates, me):
    out = []
    mine = (2 * me + jnp.arange(2)).astype(jnp.float32)
    hit = codes[:, None].astype(jnp.float32) == mine[None, :, None, None, None]
    chosen = jnp.sum(hit.astype(jnp.float32), axis=2)
    weight = jnp.sum(jnp.where(hit, gates[:, None].astype(jnp.float32), 0.0), axis=2)
    before = jnp.triu(jnp.ones((CT, CT), jnp.bfloat16), 1)
    rank = jnp.einsum(
        "aect,tu->aecu", chosen.astype(jnp.bfloat16), before, preferred_element_type=jnp.float32
    )
    count = jnp.sum(chosen, axis=3).astype(jnp.int32)
    end = jnp.cumsum(count, axis=0)
    begin = end - count
    off = lax.rem(begin, 16)
    base = begin - off
    pos = jnp.where(chosen > 0, rank + off[..., None].astype(jnp.float32), -1.0)
    tiles = (end[-1] + 127) // 128
    for c in range(CHUNKS):
        meta = jnp.concatenate(
            [pos[:, :, c], weight[:, :, c], jnp.zeros((NDEV, 4, CT), jnp.float32)], axis=1
        )
        out.append((base[:, :, c].T, off[:, :, c].T, tiles[:, c], meta))
    return out


def solution(mesh):
    def layer(x, expert, slot, gate, w_gate, w_up, w_down, s_gate, s_up, s_down):
        x, expert, slot, gate = x[0, 0], expert[0, 0], slot[0, 0], gate[0, 0]
        me = lax.axis_index("ep")
        core = lax.rem(me, 2)
        chip = me // 2

        code = jnp.where(slot < SLOTS, expert, 32).astype(jnp.bfloat16)
        packed = jnp.concatenate([code, gate.astype(jnp.bfloat16)], axis=1)
        packed = packed.reshape(TOK // (GROUP * CHUNKS), CHUNKS, GROUP, 2 * TOP)
        packed = packed.transpose(3, 1, 0, 2).reshape(2 * TOP, TOK)
        allm = lax.all_gather(packed, "ep", axis=0).reshape(NDEV, 2 * TOP, CHUNKS, CT)
        plan = positions(allm[:, :TOP], allm[:, TOP:], me)

        xs = x.reshape(TOK // (GROUP * CHUNKS), CHUNKS, GROUP, D)
        gathered = [
            lax.all_gather(xs[:, c].reshape(CT, D), "ep", axis=0) for c in range(CHUNKS)
        ]
        pair = [(i, i ^ 1) for i in range(NDEV)]
        groups = [[2 * k + c for k in range(CHIPS)] for c in range(2)]
        each = SFF // SB // 2
        both = jnp.concatenate([x, lax.ppermute(x, "ep", pair)], axis=0)
        start = (core * each)[None]
        acc = shared(both, s_gate, s_up, s_down, start, SA_BLOCKS)
        parts = []
        after = acc
        for c in range(CHUNKS):
            base, off, tiles, meta = plan[c]
            tokens, after = lax.optimization_barrier((gathered[c], after))
            if c == 0:
                acc = after
            else:
                parts[-1] = (after, *parts[-1][1:])
            keep, away = routed(base, off, tiles, core[None], tokens, meta, w_gate, w_up, w_down)
            got = lax.ppermute(away, "ep", pair)
            after = (keep + got.astype(jnp.float32)).astype(jnp.bfloat16)
            parts.append((after, keep, got))
        both, acc, after = lax.optimization_barrier((both, acc, after))
        parts[-1] = (after, *parts[-1][1:])
        for c in range(CHUNKS):
            back = lax.all_to_all(parts[c][0], "ep", 0, 0, axis_index_groups=groups, tiled=True)
            parts[c] = (back, *parts[c][1:])
        own, other = shared(both, s_gate, s_up, s_down, start + SA_BLOCKS, each - SA_BLOCKS, acc)
        other = lax.ppermute(other, "ep", pair)
        return final(chip[None], own, other, parts)[None, None]

    row = P("dp", "ep", None, None)
    return jax.shard_map(
        layer,
        mesh=mesh,
        in_specs=(row, row, row, row) + (P("ep", None, None),) * 3 + (P(None, None),) * 3,
        out_specs=row,
        check_vma=False,
    )
```

```python
import functools

import jax
import jax.numpy as jnp
from jax import lax
from jax.experimental import pallas as pl
from jax.experimental.pallas import tpu as pltpu
from jax.sharding import PartitionSpec as P


D = 3584
FF = 2560
SFF = 20480
TOP = 8
SLOTS = 80
NDEV = 16
CHIPS = 8
TOK = 256
CHUNKS = 2
CT = TOK // CHUNKS
GROUP = 8
WIN = SLOTS + 16
CAP = NDEV * SLOTS
ZROWS = CAP + 96
PASS = 6
FB = 512
NB = FF // FB
SB = 512
SA_BLOCKS = 6
VMEM = 64 * 1024 * 1024 - 65536


def shared_kernel(start_ref, x_ref, wg_ref, wu_ref, wd_ref, acc_in, *rest, last):
    j = pl.program_id(0)
    acc_ref = rest[-1]

    @pl.when(j == 0)
    def _():
        if last:
            acc_ref[...] = acc_in[...]
        else:
            acc_ref[...] = jnp.zeros_like(acc_ref)

    x = x_ref[...]
    g = jnp.dot(x, wg_ref[...], preferred_element_type=jnp.float32)
    u = jnp.dot(x, wu_ref[...], preferred_element_type=jnp.float32)
    h = (jax.nn.silu(g) * u).astype(jnp.bfloat16)
    acc_ref[...] += jnp.dot(h, wd_ref[...], preferred_element_type=jnp.float32)
    if last:
        own_ref, other_ref = rest[:2]

        @pl.when(j == pl.num_programs(0) - 1)
        def _():
            own_ref[...] = acc_ref[:TOK, :]
            other_ref[...] = acc_ref[TOK:, :].astype(jnp.bfloat16)


def shared(x, wg, wu, wd, start, count, acc=None):
    rows = 2 * TOK
    last = acc is not None
    whole = pl.BlockSpec((rows, D), lambda j, s: (0, 0))
    if last:
        acc_spec = whole
        out_specs = [pl.BlockSpec((TOK, D), lambda j, s: (0, 0))] * 2
        out_shape = [jax.ShapeDtypeStruct((TOK, D), jnp.float32), jax.ShapeDtypeStruct((TOK, D), jnp.bfloat16)]
        scratch = [pltpu.VMEM((rows, D), jnp.float32)]
    else:
        acc = jnp.zeros((8, 128), jnp.float32)
        acc_spec = pl.BlockSpec((8, 128), lambda j, s: (0, 0))
        out_specs, out_shape, scratch = whole, jax.ShapeDtypeStruct((rows, D), jnp.float32), []
    return pl.pallas_call(
        functools.partial(shared_kernel, last=last),
        grid_spec=pltpu.PrefetchScalarGridSpec(
            num_scalar_prefetch=1,
            grid=(count,),
            in_specs=[
                whole,
                pl.BlockSpec((D, SB), lambda j, s: (0, s[0] + j)),
                pl.BlockSpec((D, SB), lambda j, s: (0, s[0] + j)),
                pl.BlockSpec((SB, D), lambda j, s: (s[0] + j, 0)),
                acc_spec,
            ],
            out_specs=out_specs,
            scratch_shapes=scratch,
        ),
        out_shape=out_shape,
        compiler_params=pltpu.CompilerParams(vmem_limit_bytes=VMEM),
        cost_estimate=pl.CostEstimate(
            flops=6 * rows * D * SB * count, bytes_accessed=6 * D * SB * count, transcendentals=rows * SB * count
        ),
        name="shared",
    )(start, x, wg, wu, wd, acc)


def final_kernel(chip_ref, own_ref, other_ref, *rest):
    y_ref = rest[-1]
    chip = chip_ref[0]
    sums = []
    for c in range(CHUNKS):
        back_ref, keep_ref, got_ref = rest[3 * c : 3 * c + 3]
        t = keep_ref[0] + got_ref[0].astype(jnp.float32)
        for k in range(CHIPS):
            t += jnp.where(chip == k, 0.0, back_ref[k].astype(jnp.float32))
        sums.append(t)
    pieces = []
    for g in range(16 // GROUP):
        for c in range(CHUNKS):
            pieces.append(sums[c][g * GROUP : (g + 1) * GROUP])
    t = jnp.concatenate(pieces, axis=0)
    y_ref[...] = (t + (own_ref[...] + other_ref[...].astype(jnp.float32))).astype(jnp.bfloat16)


def final(chip, own, other, parts):
    rows = 16 * CHUNKS
    specs = [pl.BlockSpec((rows, D), lambda i, c: (i, 0))] * 2
    args = [own, other]
    for back, keep, got in parts:
        specs.append(pl.BlockSpec((CHIPS, 16, D), lambda i, c: (0, i, 0)))
        specs += [pl.BlockSpec((1, 16, D), lambda i, c: (c[0], i, 0))] * 2
        args += [back, keep, got]
    return pl.pallas_call(
        final_kernel,
        grid_spec=pltpu.PrefetchScalarGridSpec(
            num_scalar_prefetch=1,
            grid=(TOK // rows,),
            in_specs=specs,
            out_specs=pl.BlockSpec((rows, D), lambda i, c: (i, 0)),
        ),
        out_shape=jax.ShapeDtypeStruct((TOK, D), jnp.bfloat16),
        compiler_params=pltpu.CompilerParams(vmem_limit_bytes=40 * 1024 * 1024),
        cost_estimate=pl.CostEstimate(flops=20 * TOK * D, bytes_accessed=24 * CHIPS * TOK * D, transcendentals=0),
        name="final",
    )(chip, *args)


def routed_kernel(
    base_ref, off_ref, tiles_ref, core_ref, x_hbm, meta_ref, wg_ref, wu_ref, wd_ref, keep_hbm, away_hbm,
    zbuf, acc, xbuf, abuf, xsem, ksem, asem
):
    e, p, j = pl.program_id(0), pl.program_id(1), pl.program_id(2)
    mc = core_ref[0]

    def source(k, away):
        return 2 * k + (1 - mc if away else mc)

    def fetch(a, slot):
        return pltpu.make_async_copy(x_hbm.at[a], xbuf.at[slot], xsem.at[slot])

    @pl.when((e == 0) & (p == 0) & (j == 0))
    def _():
        fetch(0, 0).start()
        for q in range(2):
            tail = jnp.minimum(base_ref[q, NDEV - 1] + WIN, ZROWS - 128)
            zbuf[q, pl.ds(pl.multiple_of(tail, 16), 128), :] = jnp.zeros((128, D), jnp.bfloat16)

        def step(a, c):
            slot = lax.rem(a, 2)

            @pl.when(a < NDEV - 1)
            def _():
                fetch(a + 1, 1 - slot).start()

            fetch(a, slot).wait()
            m = meta_ref[a]
            rows = lax.broadcasted_iota(jnp.int32, (WIN, CT), 0).astype(jnp.float32)
            pick = [jnp.where(m[q : q + 1, :] == rows, 1.0, 0.0) for q in range(2)]
            pick = jnp.concatenate(pick, axis=0).astype(jnp.bfloat16)
            both = jnp.dot(pick, xbuf[slot], preferred_element_type=jnp.float32)
            row = lax.broadcasted_iota(jnp.int32, (16, 1), 0)
            for q in range(2):
                new = both[q * WIN : (q + 1) * WIN]
                base = pl.multiple_of(base_ref[q, a], 16)
                old = zbuf[q, pl.ds(base, 16), :].astype(jnp.float32)
                zbuf[q, pl.ds(base, 16), :] = jnp.where(row < off_ref[q, a], old, new[:16]).astype(jnp.bfloat16)
                zbuf[q, pl.ds(base + 16, WIN - 16), :] = new[16:].astype(jnp.bfloat16)
            return c

        lax.fori_loop(0, NDEV, step, 0)

    first = p * PASS * 128

    def ffn(start, size):
        z = zbuf[e, pl.ds(pl.multiple_of(first + start, 128), size), :]
        g = jnp.dot(z, wg_ref[0], preferred_element_type=jnp.float32)
        u = jnp.dot(z, wu_ref[0], preferred_element_type=jnp.float32)
        h = (jax.nn.silu(g) * u).astype(jnp.bfloat16)
        acc[pl.ds(start, size), :] += jnp.dot(h, wd_ref[0], preferred_element_type=jnp.float32)

    n = jnp.clip(tiles_ref[e] - p * PASS, 0, PASS)

    @pl.when(j == 0)
    def _():
        def clear(r, c):
            acc[pl.ds(pl.multiple_of(r * 128, 128), 128), :] = jnp.zeros((128, D), jnp.float32)
            return c

        lax.fori_loop(0, n, clear, 0)

    def big(r, c):
        ffn(pl.multiple_of(r * 512, 512), 512)
        return c

    lax.fori_loop(0, n // 4, big, 0)

    @pl.when(lax.rem(n // 2, 2) == 1)
    def _():
        ffn(pl.multiple_of(n // 4 * 512, 128), 256)

    @pl.when(lax.rem(n, 2) == 1)
    def _():
        ffn(pl.multiple_of((n - 1) * 128, 128), 128)

    @pl.when(j == NB - 1)
    def _():
        def keep(r, c):
            rows = acc[pl.ds(pl.multiple_of(r * 128, 128), 128), :]
            zbuf[e, pl.ds(pl.multiple_of(first + r * 128, 128), 128), :] = rows.astype(jnp.bfloat16)
            return c

        lax.fori_loop(0, n, keep, 0)

    @pl.when((e == 1) & (p == 1) & (j == NB - 1))
    def _():
        rows = lax.broadcasted_iota(jnp.int32, (WIN, CT), 0).astype(jnp.float32)

        def put_keep(k, slot):
            return pltpu.make_async_copy(acc.at[pl.ds(slot * CT, CT)], keep_hbm.at[k], ksem.at[slot])

        def put_away(k, slot):
            return pltpu.make_async_copy(abuf.at[slot], away_hbm.at[k], asem.at[slot])

        def result(a):
            m = meta_ref[a]
            total = None
            for q in range(2):
                w = jnp.where(m[q : q + 1, :] == rows, m[2 + q : 3 + q, :], 0.0).astype(jnp.bfloat16)
                base = pl.multiple_of(base_ref[q, a], 16)
                t = lax.dot_general(
                    w, zbuf[q, pl.ds(base, WIN), :], (((0,), (0,)), ((), ())), preferred_element_type=jnp.float32
                )
                total = t if total is None else total + t
            return total

        def step(k, c):
            slot = lax.rem(k, 2)

            @pl.when(k >= 2)
            def _():
                put_away(k - 2, slot).wait()
                put_keep(k - 2, slot).wait()

            abuf[slot] = result(source(k, True)).astype(jnp.bfloat16)
            put_away(k, slot).start()
            acc[pl.ds(pl.multiple_of(slot * CT, CT), CT), :] = result(source(k, False))
            put_keep(k, slot).start()
            return c

        lax.fori_loop(0, CHIPS, step, 0)
        for k in (CHIPS - 2, CHIPS - 1):
            put_away(k, k % 2).wait()
            put_keep(k, k % 2).wait()


def block(e, p, j, tiles):
    return jnp.where(tiles[e] > p * PASS, j, NB - 1)


def routed(base, off, tiles, core, x_all, meta, wg, wu, wd):
    grid_spec = pltpu.PrefetchScalarGridSpec(
        num_scalar_prefetch=4,
        grid=(2, 2, NB),
        in_specs=[
            pl.BlockSpec(memory_space=pl.ANY),
            pl.BlockSpec((NDEV, 8, CT), lambda e, p, j, *_: (0, 0, 0)),
            pl.BlockSpec((1, D, FB), lambda e, p, j, b, o, t, c: (e, 0, block(e, p, j, t))),
            pl.BlockSpec((1, D, FB), lambda e, p, j, b, o, t, c: (e, 0, block(e, p, j, t))),
            pl.BlockSpec((1, FB, D), lambda e, p, j, b, o, t, c: (e, block(e, p, j, t), 0)),
        ],
        out_specs=[pl.BlockSpec(memory_space=pl.ANY), pl.BlockSpec(memory_space=pl.ANY)],
        scratch_shapes=[
            pltpu.VMEM((2, ZROWS, D), jnp.bfloat16),
            pltpu.VMEM((PASS * 128, D), jnp.float32),
            pltpu.VMEM((2, CT, D), jnp.bfloat16),
            pltpu.VMEM((2, CT, D), jnp.bfloat16),
            pltpu.SemaphoreType.DMA((2,)),
            pltpu.SemaphoreType.DMA((2,)),
            pltpu.SemaphoreType.DMA((2,)),
        ],
    )
    return pl.pallas_call(
        routed_kernel,
        grid_spec=grid_spec,
        out_shape=[
            jax.ShapeDtypeStruct((CHIPS, CT, D), jnp.float32),
            jax.ShapeDtypeStruct((CHIPS, CT, D), jnp.bfloat16),
        ],
        compiler_params=pltpu.CompilerParams(vmem_limit_bytes=VMEM),
        cost_estimate=pl.CostEstimate(
            flops=6 * 1280 * D * FF, bytes_accessed=12 * D * FF, transcendentals=1280 * FF
        ),
        name="routed",
    )(base, off, tiles, core, x_all, meta, wg, wu, wd)


def positions(codes, gates, me):
    out = []
    mine = (2 * me + jnp.arange(2)).astype(jnp.float32)
    hit = codes[:, None].astype(jnp.float32) == mine[None, :, None, None, None]
    chosen = jnp.sum(hit.astype(jnp.float32), axis=2)
    weight = jnp.sum(jnp.where(hit, gates[:, None].astype(jnp.float32), 0.0), axis=2)
    before = jnp.triu(jnp.ones((CT, CT), jnp.bfloat16), 1)
    rank = jnp.einsum(
        "aect,tu->aecu", chosen.astype(jnp.bfloat16), before, preferred_element_type=jnp.float32
    )
    count = jnp.sum(chosen, axis=3).astype(jnp.int32)
    end = jnp.cumsum(count, axis=0)
    begin = end - count
    off = lax.rem(begin, 16)
    base = begin - off
    pos = jnp.where(chosen > 0, rank + off[..., None].astype(jnp.float32), -1.0)
    tiles = (end[-1] + 127) // 128
    for c in range(CHUNKS):
        meta = jnp.concatenate(
            [pos[:, :, c], weight[:, :, c], jnp.zeros((NDEV, 4, CT), jnp.float32)], axis=1
        )
        out.append((base[:, :, c].T, off[:, :, c].T, tiles[:, c], meta))
    return out


def solution(mesh):
    def layer(x, expert, slot, gate, w_gate, w_up, w_down, s_gate, s_up, s_down):
        x, expert, slot, gate = x[0, 0], expert[0, 0], slot[0, 0], gate[0, 0]
        me = lax.axis_index("ep")
        core = lax.rem(me, 2)
        chip = me // 2

        code = jnp.where(slot < SLOTS, expert, 32).astype(jnp.bfloat16)
        packed = jnp.concatenate([code, gate.astype(jnp.bfloat16)], axis=1)
        packed = packed.reshape(TOK // (GROUP * CHUNKS), CHUNKS, GROUP, 2 * TOP)
        packed = packed.transpose(3, 1, 0, 2).reshape(2 * TOP, TOK)
        allm = lax.all_gather(packed, "ep", axis=0).reshape(NDEV, 2 * TOP, CHUNKS, CT)
        plan = positions(allm[:, :TOP], allm[:, TOP:], me)

        xs = x.reshape(TOK // (GROUP * CHUNKS), CHUNKS, GROUP, D)
        gathered = [
            lax.all_gather(xs[:, c].reshape(CT, D), "ep", axis=0) for c in range(CHUNKS)
        ]
        pair = [(i, i ^ 1) for i in range(NDEV)]
        groups = [[2 * k + c for k in range(CHIPS)] for c in range(2)]
        each = SFF // SB // 2
        both = jnp.concatenate([x, lax.ppermute(x, "ep", pair)], axis=0)
        start = (core * each)[None]
        acc = shared(both, s_gate, s_up, s_down, start, SA_BLOCKS)
        parts = []
        after = acc
        for c in range(CHUNKS):
            base, off, tiles, meta = plan[c]
            tokens, after = lax.optimization_barrier((gathered[c], after))
            if c == 0:
                acc = after
            else:
                parts[-1] = (after, *parts[-1][1:])
            keep, away = routed(base, off, tiles, core[None], tokens, meta, w_gate, w_up, w_down)
            got = lax.ppermute(away, "ep", pair)
            after = (keep + got.astype(jnp.float32)).astype(jnp.bfloat16)
            parts.append((after, keep, got))
        both, acc, after = lax.optimization_barrier((both, acc, after))
        parts[-1] = (after, *parts[-1][1:])
        for c in range(CHUNKS):
            back = lax.all_to_all(parts[c][0], "ep", 0, 0, axis_index_groups=groups, tiled=True)
            parts[c] = (back, *parts[c][1:])
        own, other = shared(both, s_gate, s_up, s_down, start + SA_BLOCKS, each - SA_BLOCKS, acc)
        other = lax.ppermute(other, "ep", pair)
        return final(chip[None], own, other, parts)[None, None]

    row = P("dp", "ep", None, None)
    return jax.shard_map(
        layer,
        mesh=mesh,
        in_specs=(row, row, row, row) + (P("ep", None, None),) * 3 + (P(None, None),) * 3,
        out_specs=row,
        check_vma=False,
    )
```
